512 devices in a mesh: seq: 4 (over z_lo, core), exp: 32 (over x, y), ff: 4 (over z_hi).
Axes of the slice: x: 4, y: 8, z: 8 (z_hi: 4, z_lo: 2; z = z_hi * 2 + z_lo), core: 2. Of those that a mesh axis runs over, the one named last changes fastest.
Arguments:
- query_proj: bfloat16 [32, 512, 2560], P('exp', 'seq', 'ff'), may hold values from -85 to 85
- key_proj: bfloat16 [32, 512, 512], P('exp', 'seq', 'ff'), may hold values from -4.2 to 4.2
- value_proj: bfloat16 [32, 512, 512], P('exp', 'seq', 'ff'), may hold values from -6 to 6
- residual: bfloat16 [32, 512, 2560], P('exp', 'seq', 'ff'), may hold values from -60 to 60
- norm_gain: float32 [2560], P('ff'), may hold values from 0.5 to 2
- router_logit: float32 [32, 512], P('exp', 'seq'), may hold values from 1 to 6
- expert_ids: int32 [32, 512, 1], P('exp', 'seq'), may hold values from 0 to 31; in each aligned block of 128 rows (0 to 127, 128 to 255, ..., all dimensions but the last counted through in order) at most 6 rows name the same one
- gate_weight: bfloat16 [32, 2560, 4096], P('exp', None, ('seq', 'ff')), may hold values from -0.125 to 0.125
- up_weight: bfloat16 [32, 2560, 4096], P('exp', None, ('seq', 'ff')), may hold values from -0.125 to 0.125
- down_weight: bfloat16 [32, 4096, 2560], P('exp', ('seq', 'ff')), may hold values from -0.125 to 0.125
Outputs:
- layer_out: bfloat16 [32, 512, 2560], P('exp', 'seq', 'ff')
The draws below stay inside these ranges and needn't reach their ends.
Inputs may be any that keep to these rules, and one draw needn't show every extreme that they name: `expert_ids`: within each aligned block of 128 positions of a span (the positions of one index of seq), no expert is named by more than 6 tokens, and in some blocks an expert is named by exactly 6.
All inputs are finite; a program needn't handle non-finite values.
Results may differ from the reference program's by a relative error of at most 0.015.
Values may be sent and summed in bfloat16 or wider, within the bound.
A program may use at most 64 MiB of HBM per device.

```python
import math
import jax
import jax.numpy as jnp
import numpy as np
from jax import lax

HD = 128
HEADS = 20
KVH = 4
D = 2560
FF = 4096
SHARD = 128
SPAN = 512
SPANS = 32
EXPERTS = 32
CAP = 6
N_SEQ = 4
N_FF = 4


def base_keys(key):
    rows = jnp.clip(jax.random.normal(jax.random.fold_in(key, 101), (SPANS, SPAN, KVH * HD), jnp.float32), -4.0, 4.0)
    return rows


def draw_key_proj(key, part):
    return base_keys(key).astype(jnp.bfloat16)


def draw_query_proj(key, part):
    rows = jnp.clip(jax.random.normal(jax.random.fold_in(key, 103), (SPANS, SPAN, HEADS * HD), jnp.float32), -4.0, 4.0)
    return rows.astype(jnp.bfloat16)


def draw_residual(key, part):
    base = jnp.clip(jax.random.normal(jax.random.fold_in(key, 105), (SPANS, SPAN, D), jnp.float32), -5.0, 5.0)
    row_scale = jnp.exp(jax.random.uniform(jax.random.fold_in(key, 106), (SPANS, SPAN, 1), jnp.float32, -1.15, 1.15))
    direction = jnp.where(jax.random.uniform(jax.random.fold_in(key, 107), (), jnp.float32) < 0.5, -1.0, 1.0)
    ramp = jnp.linspace(-1.0, 1.0, D)[None, None, :]
    jitter = jax.random.uniform(jax.random.fold_in(key, 108), (1, 1, D), jnp.float32, -0.4, 0.4)
    col_scale = jnp.exp(0.9 * direction * ramp + jitter)
    return (base * row_scale * col_scale).astype(jnp.bfloat16)


def strengthened(drawn, rng, source, target, shards_of, factor):
    def block_of(dim):
        return (jnp.arange(drawn.shape[dim]) // (drawn.shape[dim] // shards_of)).reshape((-1,) + (1,) * (drawn.ndim - 1 - dim))

    near = jax.random.permutation(rng, shards_of)[block_of(target)]
    far = (block_of(target) + shards_of // 2) % shards_of
    return jnp.where((block_of(source) == near) | (block_of(source) == far), factor * drawn, drawn)


def block_scale(stream_key, extent, cuts, least, high):
    def one(dim, blocks):
        steps = jax.random.uniform(jax.random.fold_in(jax.random.fold_in(stream_key, 6), dim), (blocks,), jnp.float32, least / len(cuts), high / len(cuts))
        return jnp.repeat(jnp.exp(steps), extent[dim] // blocks).reshape((-1,) + (1,) * (len(extent) - dim - 1))

    gain = one(*cuts[0])
    for cut in cuts[1:]:
        gain = gain * one(*cut)
    return gain


def deal_out(rng, own, number, rows, amount, top, most, skew):
    order = jax.random.permutation(rng, amount)
    heavy_load, ordinary = portions_of(amount, rows * top, most, skew, True), portions_of(amount, rows * top, most, skew, False)
    places = jnp.arange(amount)

    def named(sizes, turn):
        used = int((sizes > 0).sum())
        fixed = max(1, used // 4)
        shifted = fixed + (places - fixed + turn * (used - fixed)) % max(1, amount - fixed)
        return jnp.zeros((amount,), jnp.int32).at[order[jnp.where(places < fixed, places, shifted)]].set(jnp.asarray(sizes, jnp.int32))

    sizes = jnp.where(number % 4 == 0, named(heavy_load, number // 4), named(ordinary, number - number // 4 - 1))
    mixed = jax.random.permutation(jax.random.fold_in(own, 3), amount)
    giver, receiver = mixed[0:amount // 2 * 2:2], mixed[1:amount // 2 * 2:2]
    room = jnp.minimum(sizes[giver] - 1, most - sizes[receiver]) // 2
    room = jnp.where((giver == order[0]) | (receiver == order[0]) | (sizes[receiver] == 0), 0, jnp.maximum(room, 0))
    shifted = jax.random.randint(jax.random.fold_in(own, 4), (amount // 2,), 0, 1 << 20) % (room + 1)
    sizes = sizes.at[giver].add(-shifted).at[receiver].add(shifted)
    labels = jnp.searchsorted(jnp.cumsum(sizes), jnp.arange(rows * top), side="right").astype(jnp.int32)
    table = labels.reshape(top, rows).T
    table = table[jax.random.permutation(jax.random.fold_in(own, 1), rows)]
    turn = jax.random.randint(jax.random.fold_in(own, 2), (rows, 1), 0, top)
    return jnp.take_along_axis(table, (jnp.arange(top)[None, :] + turn) % top, axis=1)


def portions_of(count, total, bound, skew, full):
    portions = [(1 << 20) // math.isqrt(standing ** skew) + 1 for standing in range(1, count + 1)]
    largest = bound if full else min(bound, max(-(-total // count), total * portions[0] // sum(portions)))
    least = 1 if total - largest >= count - 1 else 0
    given, surplus = [largest] + [least] * (count - 1), total - largest - least * (count - 1)
    while surplus > 0:
        candidates = [i for i in range(1, count) if given[i] < largest] or [i for i in range(1, count) if given[i] < bound]
        pool, budget = sum([portions[i] for i in candidates]), surplus
        for i in candidates:
            extra = min(bound - given[i], max(1, budget * portions[i] // pool), surplus)
            given[i] = given[i] + extra
            surplus = surplus - extra
    return np.array(given)


def scatter_about(key, dims, spread, bound, shards=(), kind=jnp.bfloat16):
    array = spread * jax.random.normal(key, dims, jnp.float32)
    if shards:
        array = array * block_scale(key, dims, shards, -0.22, 0.18)
    return jnp.clip(array, -bound, bound).astype(kind)


def gaussian_with(stream_key, dims, width, most, cuts, heavy, kind=jnp.bfloat16):
    values = width * jax.random.normal(stream_key, dims, jnp.float32)
    if cuts:
        values = values * block_scale(stream_key, dims, cuts, -0.22, 0.18)
    return jnp.clip(strengthened(values, jax.random.fold_in(stream_key, 3), *heavy), -most, most).astype(kind)


def setup_inputs(seed: int = 0) -> dict:
    seeds = jax.random.split(jax.random.key(seed), 11)
    query_proj = draw_query_proj(jax.random.fold_in(seeds[10], 71), 0)
    key_proj = draw_key_proj(jax.random.fold_in(seeds[10], 71), 0)
    value_proj = scatter_about(seeds[2], (SPANS, SPAN, KVH * HD), 1.0, 6.0, ((0, 32), (1, 4), (2, 4)))
    residual = draw_residual(jax.random.fold_in(seeds[10], 71), 0)
    norm_gain = jnp.clip(jnp.exp(math.log(2.0) - 1.3862944 * jax.random.uniform(seeds[4], (D,), jnp.float32) ** block_scale(seeds[4], (D,), ((0, 4),), -0.2, 0.2)), 0.5, 2.0)
    router_logit = jnp.clip(1.0 + 5.0 * jax.random.uniform(seeds[5], (SPANS, SPAN), jnp.float32) ** block_scale(seeds[5], (SPANS, SPAN), ((0, 32), (1, 4)), -0.2, 0.2), 1.0, 6.0)
    expert_ids_keys = jax.random.split(jax.random.fold_in(seeds[6], 1), SPANS * SPAN // SHARD)
    expert_ids_turns = jax.random.permutation(jax.random.fold_in(seeds[6], 3), SPANS * SPAN // SHARD)
    expert_ids = jax.vmap(lambda own, number: deal_out(jax.random.fold_in(seeds[6], 2), own, number, SHARD, EXPERTS, 1, CAP, 2))(expert_ids_keys, expert_ids_turns).reshape((SPANS, SPAN, 1))
    gate_weight = scatter_about(seeds[7], (EXPERTS, D, FF), D ** -0.5, 0.125, ((0, 32), (2, 16)))
    up_weight = scatter_about(seeds[8], (EXPERTS, D, FF), D ** -0.5, 0.125, ((0, 32), (2, 16)))
    down_weight = gaussian_with(seeds[9], (EXPERTS, FF, D), FF ** -0.5, 0.125, ((0, 32), (1, 16)), (1, 2, 16, 2.0))
    return {"query_proj": query_proj, "key_proj": key_proj, "value_proj": value_proj, "residual": residual, "norm_gain": norm_gain, "router_logit": router_logit, "expert_ids": expert_ids, "gate_weight": gate_weight, "up_weight": up_weight, "down_weight": down_weight}


floor_score = -1e+30
norm_eps = 1e-05

def span_attention(pieces):
    queries, keys_in, values_in = pieces
    group = HEADS // KVH
    query_f = queries.astype(jnp.float32).reshape(SPAN, KVH, group, HD)
    key_f = keys_in.astype(jnp.float32).reshape(SPAN, KVH, HD)
    value_f = values_in.astype(jnp.float32).reshape(SPAN, KVH, HD)
    scores = jnp.einsum('qagd,kad->agqk', query_f, key_f, precision=lax.Precision.HIGHEST) * HD ** (-0.5)
    positions = lax.iota(jnp.int32, SPAN)
    allowed = positions[None, :] <= positions[:, None]
    masked = jnp.where(allowed, scores, floor_score)
    peak = lax.optimization_barrier(jnp.max(masked, axis=-1))
    weights = jnp.where(allowed, jnp.exp(masked - peak[..., None]), 0.0)
    rounded = lax.optimization_barrier(weights.astype(jnp.bfloat16)).astype(jnp.float32)
    mixed = jnp.einsum('agqk,kad->agqd', rounded, value_f, precision=lax.Precision.HIGHEST)
    mixed = mixed / lax.optimization_barrier(jnp.sum(weights, axis=-1))[..., None]
    return mixed.transpose(2, 0, 1, 3).reshape(SPAN, HEADS * HD)

def reference(query_proj, key_proj, value_proj, residual, norm_gain, router_logit, expert_ids, gate_weight, up_weight, down_weight):
    attention = lax.map(span_attention, (query_proj, key_proj, value_proj))
    stream = (residual.astype(jnp.float32) + attention).astype(jnp.bfloat16)
    stream_f = stream.astype(jnp.float32)
    meansq = lax.optimization_barrier(jnp.mean(stream_f * stream_f, axis=-1))
    routed_in = stream_f * lax.rsqrt(meansq + norm_eps)[..., None] * norm_gain * jax.nn.sigmoid(router_logit)[..., None]
    routed_in = routed_in.astype(jnp.bfloat16)
    route = expert_ids[..., 0]
    onehot = (route[..., None] == jnp.arange(EXPERTS, dtype=jnp.int32)).astype(jnp.float32)
    blocks = onehot.reshape(SPANS, N_SEQ, SHARD, EXPERTS)
    earlier = jnp.cumsum(blocks, axis=2) - blocks
    slot = lax.optimization_barrier(jnp.sum(earlier * blocks, axis=-1)).astype(jnp.int32)
    span_index = jnp.arange(SPANS, dtype=jnp.int32)[:, None, None]
    shard_index = jnp.arange(N_SEQ, dtype=jnp.int32)[None, :, None]
    position = ((shard_index * EXPERTS + span_index) * CAP + slot).reshape(-1)
    route_flat = route.reshape(-1)
    routed_flat = routed_in.reshape(-1, D)
    rows_all = N_SEQ * EXPERTS * CAP
    groups = N_SEQ * N_FF
    unit_count = FF // groups

    def expert_output(expert):
        slot_index = jnp.where(route_flat == expert, position, rows_all)
        buffer = jnp.zeros((rows_all, D), jnp.bfloat16).at[slot_index].set(routed_flat, mode='drop')
        gate = jnp.dot(buffer, gate_weight[expert], preferred_element_type=jnp.float32)
        upward = jnp.dot(buffer, up_weight[expert], preferred_element_type=jnp.float32)
        activated = (jax.nn.silu(gate) * upward).astype(jnp.bfloat16)
        parts = jnp.einsum('rgk,gkd->grd', activated.astype(jnp.float32).reshape(rows_all, groups, unit_count), down_weight[expert].astype(jnp.float32).reshape(groups, unit_count, D), precision=lax.Precision.HIGHEST)
        parts = lax.optimization_barrier(parts.astype(jnp.bfloat16)).astype(jnp.float32)
        return lax.optimization_barrier(jnp.sum(parts, axis=0)).astype(jnp.bfloat16)
    expert_all = lax.map(expert_output, jnp.arange(EXPERTS, dtype=jnp.int32))
    picked = expert_all[route_flat, position]
    layer_out = stream_f.reshape(-1, D) + picked.astype(jnp.float32)
    return layer_out.astype(jnp.bfloat16).reshape(SPANS, SPAN, D)
```

```python
import jax
import jax.numpy as jnp
from jax import lax
from jax.experimental import pallas as pl
from jax.experimental.pallas import tpu as pltpu
from jax.sharding import Mesh
from jax.sharding import PartitionSpec as P

HD = 128
HEADS = 20
KVH = 4
D = 2560
CAP = 6
PAD = 8
SEQ = ("zl", "core")
SEQ_FF = ("zl", "core", "ff")
NORM_EPS = 1e-05
FLOOR = -1e30
BF16 = jnp.bfloat16
F32 = jnp.float32
MESH = pl.DeviceIdType.MESH


def remote(src, dst, send, recv, where):
    return pltpu.make_async_remote_copy(
        src_ref=src, dst_ref=dst, send_sem=send, recv_sem=recv, device_id=where, device_id_type=MESH
    )


def dot(a, b):
    return jnp.dot(a, b, preferred_element_type=F32)


def dot_rows(a, b):
    return lax.dot_general(a, b, (((0,), (0,)), ((), ())), preferred_element_type=F32)


def dot_cols(a, b):
    return lax.dot_general(a, b, (((1,), (1,)), ((), ())), preferred_element_type=F32)


def iota(shape, dim):
    return lax.broadcasted_iota(jnp.int32, shape, dim)


def as_column(row):
    n = row.shape[-1]
    eye = iota((n, n), 0) == iota((n, n), 1)
    return jnp.sum(jnp.where(eye, jnp.broadcast_to(row, (n, n)), 0.0), axis=1, keepdims=True)


def kv_kernel(k_ref, v_ref, k_out, v_out, send_sem, recv_sem):
    zl, core = lax.axis_index("zl"), lax.axis_index("core")
    me = zl * 2 + core
    peers = (
        {"zl": 1 - zl, "core": core},
        {"zl": 1 - zl, "core": 1 - core},
        {"core": 1 - core},
    )
    barrier = pltpu.get_barrier_semaphore()
    for where in peers:
        pl.semaphore_signal(barrier, inc=1, device_id=where, device_id_type=MESH)
    k_out[me] = k_ref[...]
    v_out[me] = v_ref[...]
    pl.semaphore_wait(barrier, 3)
    copies = []
    for n, (src, dst) in enumerate(((k_ref, k_out), (v_ref, v_out))):
        for p, where in enumerate(peers):
            copies.append(remote(src, dst.at[me], send_sem.at[n, p], recv_sem.at[n, p], where))
            copies[-1].start()
    for copy in copies:
        copy.wait()


def gather_kv(key, value):
    rows, width = key.shape
    vmem = pl.BlockSpec(memory_space=pltpu.VMEM)
    shape = jax.ShapeDtypeStruct((4, rows, width), key.dtype)
    return pl.pallas_call(
        kv_kernel,
        out_shape=(shape, shape),
        in_specs=[vmem] * 2,
        out_specs=(vmem, vmem),
        scratch_shapes=[pltpu.SemaphoreType.DMA((2, 3)), pltpu.SemaphoreType.DMA((2, 3))],
        compiler_params=pltpu.CompilerParams(collective_id=0, has_side_effects=True),
        name="gather_kv",
    )(key, value)


def layer_kernel(
    n_exp,
    n_ff,
    q_ref,
    k_ref,
    v_ref,
    res_ref,
    gain_ref,
    logit_ref,
    ids_ref,
    wg_hbm,
    wu_hbm,
    wd_hbm,
    out_ref,
    wg_raw,
    wu_raw,
    wd,
    wgu,
    stream,
    sel,
    packed,
    landed,
    gains,
    sigs,
    xbuf,
    acc,
    sq,
    act,
    sib_out,
    sib_in,
    rs_out,
    rs_in,
    back_out,
    back_in,
    w_sem,
    gain_send,
    gain_recv,
    a2a_send,
    a2a_recv,
    sig_send,
    sig_recv,
    ag_send,
    ag_recv,
    own_send,
    own_recv,
    fwd_send,
    fwd_recv,
    sp_send,
    sp_recv,
    rs_send,
    rs_recv,
    bk_send,
    bk_recv,
):
    n_ring = 2 * n_ff
    items = n_ring - 1
    zl, core = lax.axis_index("zl"), lax.axis_index("core")
    exp, ff = lax.axis_index("exp"), lax.axis_index("ff")
    shard = zl * 2 + core
    zeta = ff * 2 + zl
    tokens, width = q_ref.shape
    slots = n_exp * PAD
    rows = n_exp * CAP
    half = rows // 2
    hidden = wg_raw.shape[1]

    def at_ring(step):
        z = lax.rem(zeta + step + n_ring, n_ring)
        return {"zl": lax.rem(z, 2), "ff": z // 2}

    sibling = {"core": 1 - core}
    seq_peers = (sibling, {"zl": 1 - zl}, {"zl": 1 - zl, "core": 1 - core})
    nxt = (at_ring(1), at_ring(-1))

    barrier = pltpu.get_barrier_semaphore()

    def greet(k, carry):
        pl.semaphore_signal(
            barrier, inc=1, device_id={"exp": lax.rem(exp + k, n_exp)}, device_id_type=MESH
        )
        return carry

    lax.fori_loop(1, n_exp, greet, 0)
    greeted = [sibling, {"zl": 1 - zl, "core": 1 - core}, *nxt]
    ff_peers = [{"ff": lax.rem(ff + k, n_ff)} for k in range(1, n_ff)]
    for where in greeted + ff_peers:
        pl.semaphore_signal(barrier, inc=1, device_id=where, device_id_type=MESH)

    loads = [
        pltpu.make_async_copy(src, dst, w_sem.at[n])
        for n, (src, dst) in enumerate(((wg_hbm, wg_raw), (wu_hbm, wu_raw), (wd_hbm, wd)))
    ]
    for load in loads:
        load.start()

    kv_local = k_ref.shape[2] // HD
    group = HEADS // KVH
    span = 4 * tokens
    for a in range(kv_local):
        keys = k_ref[:, :, a * HD : (a + 1) * HD].reshape(span, HD)
        values = v_ref[:, :, a * HD : (a + 1) * HD].reshape(span, HD)
        allowed = iota((tokens, span), 1) <= iota((tokens, span), 0) + shard * tokens
        for g in range(group):
            h = (a * group + g) * HD
            scores = dot_cols(q_ref[:, h : h + HD], keys) * HD ** (-0.5)
            scores = jnp.where(allowed, scores, FLOOR)
            peak = jnp.max(scores, axis=-1, keepdims=True)
            weights = jnp.where(allowed, jnp.exp(scores - peak), 0.0)
            total = jnp.sum(weights, axis=-1, keepdims=True)
            mixed = dot(weights.astype(BF16), values) / total
            stream[:, h : h + HD] = (res_ref[:, h : h + HD].astype(F32) + mixed).astype(BF16)

    route = as_column(ids_ref[...].astype(F32))
    onehot = (route == iota((tokens, HD), 1).astype(F32)).astype(F32)
    below = (iota((tokens, tokens), 0) > iota((tokens, tokens), 1)).astype(BF16)
    earlier = dot(below, onehot.astype(BF16))
    slot = jnp.sum(earlier * onehot, axis=1, keepdims=True)
    lane = iota((tokens, slots), 1).astype(F32)
    pick = (lane == route * PAD + slot).astype(BF16)
    sel[...] = pick
    gate_in = as_column(jax.nn.sigmoid(logit_ref[...]))
    gate_hi = gate_in.astype(BF16)
    gate_lo = (gate_in - gate_hi.astype(F32)).astype(BF16)
    at_slot = slot == iota((tokens, HD), 1).astype(F32)
    meta = dot_rows(
        (lane == route * PAD + CAP).astype(BF16), jnp.where(at_slot, gate_hi.astype(F32), 0.0).astype(BF16)
    ) + dot_rows(
        (lane == route * PAD + (CAP + 1)).astype(BF16),
        jnp.where(at_slot, gate_lo.astype(F32), 0.0).astype(BF16),
    )
    for c in range(0, width, HD):
        block = dot_rows(pick, stream[:, c : c + HD])
        if c == 0:
            block = block + meta
        packed[:, :, c : c + HD] = block.astype(BF16).reshape(n_exp, PAD, HD)
    landed[exp] = packed[exp]
    gains[ff] = gain_ref[...]
    acc[...] = jnp.zeros_like(acc)
    sq[...] = jnp.zeros_like(sq)

    pl.semaphore_wait(barrier, n_exp - 1 + len(greeted) + len(ff_peers))

    def gain_copy(k):
        return remote(
            gains.at[ff], gains.at[ff], gain_send.at[k], gain_recv.at[k], ff_peers[k]
        )

    for k in range(n_ff - 1):
        gain_copy(k).start()

    def a2a_copy(k):
        to = lax.rem(exp + k, n_exp)
        return remote(
            packed.at[to], landed.at[exp], a2a_send.at[k - 1], a2a_recv.at[k - 1], {"exp": to}
        )

    def a2a_start(k, carry):
        a2a_copy(k).start()
        return carry

    lax.fori_loop(1, n_exp, a2a_start, 0)

    for load in loads:
        load.wait()
    for k in range(n_ff - 1):
        gain_copy(k).wait_recv()

    cols = width // HD

    def fold(b, carry):
        f = b // cols
        r = b - f * cols
        column = as_column(gains[f, pl.ds(r, 1), :])
        src = pl.ds(pl.multiple_of(b * HD, HD), HD)
        dst = pl.ds(pl.multiple_of(r * HD, HD), HD)
        wgu[f, dst, 0:hidden] = (wg_raw[src, :].astype(F32) * column).astype(BF16)
        wgu[f, dst, hidden : 2 * hidden] = (wu_raw[src, :].astype(F32) * column).astype(BF16)
        return carry

    lax.fori_loop(0, n_ff * cols, fold, 0)

    def a2a_wait(k, carry):
        a2a_copy(k).wait_recv()
        return carry

    lax.fori_loop(1, n_exp, a2a_wait, 0)

    q_col = iota((rows, slots), 1)
    keep = (iota((rows, slots), 0) == q_col - 2 * (q_col >> 3)) & ((q_col & 7) < CAP)
    keep = keep.astype(BF16)
    for c in range(0, width, HD):
        whole = landed[:, :, c : c + HD].reshape(slots, HD)
        dense = dot(keep, whole).astype(BF16)
        xbuf[zeta, core, 0, :, c : c + HD] = dense[:half]
        xbuf[zeta, core, 1, :, c : c + HD] = dense[half:]
        if c == 0:
            q_m = iota((2 * n_exp, slots), 1)
            pick_m = (iota((2 * n_exp, slots), 0) == (q_m >> 3) * 2 + (q_m & 7) - CAP) & ((q_m & 7) >= CAP)
            sigs[shard] = dot(pick_m.astype(BF16), whole).astype(BF16)

    def ring_item(d, j):
        z = zeta - (j // 2 + 1) if d == 0 else zeta + (j // 2 + 1)
        z = lax.rem(z + n_ring, n_ring)
        h = lax.rem(j, 2) if d == 0 else 1 - lax.rem(j, 2)
        return z, h

    def ag_copy(d, j, z, h):
        return remote(
            xbuf.at[z, core, h], xbuf.at[z, core, h], ag_send.at[d, j], ag_recv.at[d, j], nxt[d]
        )

    def own_copy(h):
        return remote(
            xbuf.at[zeta, core, h], xbuf.at[zeta, core, h], own_send.at[h], own_recv.at[h], sibling
        )

    def fwd_copy(d, j, z, h):
        return remote(
            xbuf.at[z, core, h], xbuf.at[z, core, h], fwd_send.at[d, j], fwd_recv.at[d, j], sibling
        )

    def sib_fwd(d, j, z, h):
        return remote(
            xbuf.at[z, 1 - core, h], xbuf.at[z, 1 - core, h], fwd_send.at[d, j], fwd_recv.at[d, j], sibling
        )

    for n in range(2):
        for d in range(2):
            ag_copy(d, n, zeta, n if d == 0 else 1 - n).start()
    for h in range(2):
        own_copy(h).start()
    sig_copies = [
        remote(sigs.at[shard], sigs.at[shard], sig_send.at[p], sig_recv.at[p], where)
        for p, where in enumerate(seq_peers)
    ]
    for copy in sig_copies:
        copy.start()

    def multiply(z, c, h):
        x = xbuf[z, c, h]
        s = lax.rem(z, 2) * 2 + c
        acc[s, h] += dot(x, wgu[z // 2])
        squares = None
        for b in range(cols):
            xf = x[:, b * HD : (b + 1) * HD].astype(F32)
            squares = xf * xf if squares is None else squares + xf * xf
        sq[s, h] += squares

    for h in range(2):
        multiply(zeta, core, h)
    for h in range(2):
        remote(
            xbuf.at[zeta, 1 - core, h], xbuf.at[zeta, 1 - core, h], own_send.at[h], own_recv.at[h], sibling
        ).wait_recv()
    for h in range(2):
        multiply(zeta, 1 - core, h)

    def gather_step(j, carry):
        for d in range(2):
            z, h = ring_item(d, j)
            ag_copy(d, j, z, h).wait_recv()

            @pl.when(j < items - 2)
            def _():
                ag_copy(d, j + 2, z, h).start()

            fwd_copy(d, j, z, h).start()
        for d in range(2):
            z, h = ring_item(d, j)
            multiply(z, core, h)
        for d in range(2):
            z, h = ring_item(d, j)
            sib_fwd(d, j, z, h).wait_recv()
            multiply(z, 1 - core, h)
        return carry

    lax.fori_loop(0, items, gather_step, 0)

    for copy in sig_copies:
        copy.wait_recv()

    for h in range(2):
        r_row = iota((half, 2 * n_exp), 0) + h * half
        first = 6 * (iota((half, 2 * n_exp), 1) >> 1)
        spread = ((r_row >= first) & (r_row < first + CAP)).astype(BF16)
        r_lane = iota((half, HD), 0) + h * half
        r_slot = r_lane - CAP * ((r_lane * 683) >> 12)
        here = r_slot == iota((half, HD), 1)
        for s in range(4):
            sig = jnp.sum(jnp.where(here, dot(spread, sigs[s]), 0.0), axis=1, keepdims=True)
            meansq = jnp.sum(sq[s, h], axis=1, keepdims=True) / D
            factor = lax.rsqrt(meansq + NORM_EPS) * sig
            gate = acc[s, h, :, 0:hidden] * factor
            up = acc[s, h, :, hidden : 2 * hidden] * factor
            act[s, h] = (gate / (1.0 + jnp.exp(-gate)) * up).astype(BF16)

    def partial(z, c, h):
        s = lax.rem(z, 2) * 2 + c
        return dot(act[s, h], wd[:, pl.ds(pl.multiple_of((z // 2) * width, HD), width)])

    def rs_target(d, j):
        k = n_ff - (j + 1) // 2
        z = lax.rem((zeta + k if d == 0 else zeta - k) + n_ring, n_ring)
        h = lax.rem(j, 2) if d == 0 else 1 - lax.rem(j, 2)
        return z, h

    def sp_copy(d, j):
        return remote(
            sib_out.at[d, j], sib_in.at[d, j], sp_send.at[d, j], sp_recv.at[d, j], sibling
        )

    def for_sibling(j):
        for d in range(2):
            z, h = rs_target(d, j)
            sib_out[d, j] = partial(z, 1 - core, h).astype(BF16)
        for d in range(2):
            sp_copy(d, j).start()

    def rs_copy(d, j):
        return remote(rs_out.at[d, j], rs_in.at[d, j], rs_send.at[d, j], rs_recv.at[d, j], nxt[d])

    def scatter_step(j, carry):
        @pl.when(j < items - 1)
        def _():
            for_sibling(j + 1)

        for d in range(2):
            z, h = rs_target(d, j)
            mine = partial(z, core, h)
            sp_copy(d, j).wait_recv()
            rs_out[d, j] = (mine + sib_in[d, j].astype(F32)).astype(BF16)

            @pl.when(j >= 2)
            def _():
                rs_copy(d, j - 2).wait_recv()
                rs_out[d, j] = (mine + sib_in[d, j].astype(F32) + rs_in[d, j - 2].astype(F32)).astype(BF16)

        for d in range(2):
            rs_copy(d, j).start()
        return carry

    for_sibling(0)
    lax.fori_loop(0, items, scatter_step, 0)
    for h in range(2):
        sib_out[h, items] = partial(zeta, 1 - core, h).astype(BF16)
    for h in range(2):
        sp_copy(h, items).start()
    finals = [partial(zeta, core, h) for h in range(2)]
    for h in range(2):
        sp_copy(h, items).wait_recv()
        finals[h] = finals[h] + sib_in[h, items].astype(F32)
    for j in (items - 2, items - 1):
        for d in range(2):
            h = j % 2 if d == 0 else 1 - j % 2
            rs_copy(d, j).wait_recv()
            finals[h] = finals[h] + rs_in[d, j].astype(F32)
    result = jnp.concatenate([f.astype(BF16) for f in finals], axis=0)

    q_row = iota((slots, rows), 0)
    spread = (iota((slots, rows), 1) == q_row - 2 * (q_row >> 3)) & ((q_row & 7) < CAP)
    spread = spread.astype(BF16)
    for c in range(0, width, HD):
        back_out[:, :, c : c + HD] = (
            dot(spread, result[:, c : c + HD]).astype(BF16).reshape(n_exp, PAD, HD)
        )
    back_in[exp] = back_out[exp]

    def bk_copy(k):
        to = lax.rem(exp + k, n_exp)
        return remote(
            back_out.at[to], back_in.at[exp], bk_send.at[k - 1], bk_recv.at[k - 1], {"exp": to}
        )

    def bk_start(k, carry):
        bk_copy(k).start()
        return carry

    def bk_wait(k, carry):
        bk_copy(k).wait_recv()
        return carry

    lax.fori_loop(1, n_exp, bk_start, 0)

    for k in range(n_ff - 1):
        gain_copy(k).wait_send()
    for copy in sig_copies:
        copy.wait_send()
    for h in range(2):
        own_copy(h).wait_send()
        sp_copy(h, items).wait_send()

    def drain(j, carry):
        for d in range(2):
            ag_copy(d, j, zeta, 0).wait_send()
            fwd_copy(d, j, zeta, 0).wait_send()
            sp_copy(d, j).wait_send()
            rs_copy(d, j).wait_send()
        return carry

    lax.fori_loop(0, items, drain, 0)

    def drain_a2a(k, carry):
        a2a_copy(k).wait_send()
        return carry

    lax.fori_loop(1, n_exp, drain_a2a, 0)
    lax.fori_loop(1, n_exp, bk_wait, 0)
    for c in range(0, width, HD):
        picked = dot(sel[...], back_in[:, :, c : c + HD].reshape(slots, HD))
        out_ref[:, c : c + HD] = (stream[:, c : c + HD].astype(F32) + picked).astype(BF16)

    def drain_bk(k, carry):
        bk_copy(k).wait_send()
        return carry

    lax.fori_loop(1, n_exp, drain_bk, 0)


def run_layer(n_exp, n_ff, query, keys, values, residual, gain, logit, ids, wg, wu, wd):
    tokens, width = query.shape
    hidden = wg.shape[1]
    n_ring = 2 * n_ff
    items = n_ring - 1
    rows = n_exp * CAP
    half = rows // 2
    slots = n_exp * PAD
    vmem = pl.BlockSpec(memory_space=pltpu.VMEM)
    hbm = pl.BlockSpec(memory_space=pl.ANY)
    dma = pltpu.SemaphoreType.DMA

    def kernel(*refs):
        layer_kernel(n_exp, n_ff, *refs)

    return pl.pallas_call(
        kernel,
        out_shape=jax.ShapeDtypeStruct((tokens, width), BF16),
        in_specs=[vmem] * 7 + [hbm] * 3,
        out_specs=vmem,
        scratch_shapes=[
            pltpu.VMEM(wg.shape, BF16),
            pltpu.VMEM(wu.shape, BF16),
            pltpu.VMEM(wd.shape, BF16),
            pltpu.VMEM((n_ff, width, 2 * hidden), BF16),
            pltpu.VMEM((tokens, width), BF16),
            pltpu.VMEM((tokens, slots), BF16),
            pltpu.VMEM((n_exp, PAD, width), BF16),
            pltpu.VMEM((n_exp, PAD, width), BF16),
            pltpu.VMEM((n_ff, *gain.shape), F32),
            pltpu.VMEM((4, 2 * n_exp, HD), BF16),
            pltpu.VMEM((n_ring, 2, 2, half, width), BF16),
            pltpu.VMEM((4, 2, half, 2 * hidden), F32),
            pltpu.VMEM((4, 2, half, HD), F32),
            pltpu.VMEM((4, 2, half, hidden), BF16),
            pltpu.VMEM((2, items + 1, half, width), BF16),
            pltpu.VMEM((2, items + 1, half, width), BF16),
            pltpu.VMEM((2, items, half, width), BF16),
            pltpu.VMEM((2, items, half, width), BF16),
            pltpu.VMEM((n_exp, PAD, width), BF16),
            pltpu.VMEM((n_exp, PAD, width), BF16),
            dma((3,)),
            dma((n_ff - 1,)),
            dma((n_ff - 1,)),
            dma((n_exp - 1,)),
            dma((n_exp - 1,)),
            dma((3,)),
            dma((3,)),
            dma((2, items)),
            dma((2, items)),
            dma((2,)),
            dma((2,)),
            dma((2, items)),
            dma((2, items)),
            dma((2, items + 1)),
            dma((2, items + 1)),
            dma((2, items)),
            dma((2, items)),
            dma((n_exp - 1,)),
            dma((n_exp - 1,)),
        ],
        compiler_params=pltpu.CompilerParams(
            collective_id=1, has_side_effects=True, vmem_limit_bytes=60 * 1024 * 1024
        ),
        name="layer",
    )(query, keys, values, residual, gain, logit, ids, wg, wu, wd)


def solution(mesh):
    n_exp, n_ff = mesh.shape["exp"], mesh.shape["ff"]
    torus = Mesh(mesh.devices.reshape(2, 2, n_exp, n_ff), ("zl", "core", "exp", "ff"))

    def body(query, key, value, residual, gain, logit, ids, wg, wu, wd):
        keys, values = gather_kv(key[0], value[0])
        out = run_layer(
            n_exp,
            n_ff,
            query[0],
            keys,
            values,
            residual[0],
            gain.reshape(-1, HD),
            logit,
            ids.reshape(1, -1),
            wg[0],
            wu[0],
            wd[0],
        )
        return out[None]

    placed = (
        P("exp", SEQ, "ff"),
        P("exp", SEQ, "ff"),
        P("exp", SEQ, "ff"),
        P("exp", SEQ, "ff"),
        P("ff"),
        P("exp", SEQ),
        P("exp", SEQ, None),
        P("exp", None, SEQ_FF),
        P("exp", None, SEQ_FF),
        P("exp", SEQ_FF, None),
    )
    return jax.shard_map(
        body, mesh=torus, in_specs=placed, out_specs=P("exp", SEQ, "ff"), check_vma=False
    )
```

```python
import jax
import jax.numpy as jnp
from jax import lax
from jax.experimental import pallas as pl
from jax.experimental.pallas import tpu as pltpu
from jax.sharding import Mesh
from jax.sharding import PartitionSpec as P

HD = 128
HEADS = 20
KVH = 4
D = 2560
CAP = 6
ROWS = 16
LOT = 16
LAG = 2
SEQ = ("zl", "core")
SEQ_FF = ("zl", "core", "ff")
NORM_EPS = 1e-05
FLOOR = -1e30
BF16 = jnp.bfloat16
F32 = jnp.float32
MESH = pl.DeviceIdType.MESH


def remote(src, dst, send, recv, where):
    return pltpu.make_async_remote_copy(
        src_ref=src, dst_ref=dst, send_sem=send, recv_sem=recv, device_id=where, device_id_type=MESH
    )


def dot(a, b):
    return jnp.dot(a, b, preferred_element_type=F32)


def dot_rows(a, b):
    return lax.dot_general(a, b, (((0,), (0,)), ((), ())), preferred_element_type=F32)


def dot_cols(a, b):
    return lax.dot_general(a, b, (((1,), (1,)), ((), ())), preferred_element_type=F32)


def iota(shape, dim):
    return lax.broadcasted_iota(jnp.int32, shape, dim)


def as_column(row):
    n = row.shape[-1]
    eye = iota((n, n), 0) == iota((n, n), 1)
    return jnp.sum(jnp.where(eye, jnp.broadcast_to(row, (n, n)), 0.0), axis=1, keepdims=True)


def layer_kernel(
    n_exp,
    n_ff,
    k_hbm,
    v_hbm,
    ids_hbm,
    logit_hbm,
    gain_hbm,
    q_hbm,
    res_hbm,
    wg_hbm,
    wu_hbm,
    wd_hbm,
    out_ref,
    kbuf,
    vbuf,
    ids,
    logit,
    gains,
    query,
    res,
    wg_raw,
    wu_raw,
    wd,
    wgu,
    stream,
    choose,
    owner,
    metas,
    keep,
    widen,
    packed,
    landed,
    sigs,
    xbuf,
    acc,
    sq,
    act,
    sib_out,
    sib_in,
    rs_out,
    rs_in,
    back_out,
    back_in,
    load_sem,
    kv_send,
    kv_recv,
    few_send,
    few_recv,
    a2a_send,
    a2a_recv,
    ring_send,
    ag_recv,
    own_recv,
    fwd_recv,
    sp_recv,
    rs_recv,
    bk_send,
    bk_recv,
):
    n_ring = 2 * n_ff
    items = n_ring - 1
    zl, core = lax.axis_index("zl"), lax.axis_index("core")
    exp, ff = lax.axis_index("exp"), lax.axis_index("ff")
    shard = zl * 2 + core
    zeta = ff * 2 + zl
    tokens, width = query.shape
    cols = width // HD
    part = CAP // 2
    half = n_exp * part
    hidden = wg_raw.shape[1]
    lot = min(n_exp, LOT)

    def at_ring(step):
        z = lax.rem(zeta + step + n_ring, n_ring)
        return {"zl": lax.rem(z, 2), "ff": z // 2}

    sibling = {"core": 1 - core}
    seq_peers = ({"zl": 1 - zl, "core": 1 - core}, {"zl": 1 - zl}, sibling)
    nxt = (at_ring(1), at_ring(-1))
    ff_peers = [{"ff": lax.rem(ff + k, n_ff)} for k in range(1, n_ff)]

    loads = [
        pltpu.make_async_copy(src, dst, load_sem.at[n])
        for n, (src, dst) in enumerate(
            (
                (ids_hbm, ids),
                (logit_hbm, logit),
                (k_hbm, kbuf.at[shard]),
                (v_hbm, vbuf.at[shard]),
                (gain_hbm, gains.at[ff]),
                (q_hbm, query),
                (res_hbm, res),
                (wg_hbm, wg_raw),
                (wu_hbm, wu_raw),
                (wd_hbm, wd),
            )
        )
    ]
    for load in loads:
        load.start()
    barrier = pltpu.get_barrier_semaphore()
    greeted = [sibling, {"zl": 1 - zl, "core": 1 - core}, *nxt]
    for where in greeted + ff_peers:
        pl.semaphore_signal(barrier, inc=1, device_id=where, device_id_type=MESH)

    def greet(k, carry):
        pl.semaphore_signal(
            barrier, inc=1, device_id={"exp": lax.rem(exp + k, n_exp)}, device_id_type=MESH
        )
        return carry

    lax.fori_loop(1, n_exp, greet, 0)
    loads[2].wait()
    loads[3].wait()
    loads[4].wait()

    pl.semaphore_wait(barrier, n_exp - 1 + len(greeted) + len(ff_peers))
    for n, buf in enumerate((kbuf, vbuf)):
        for where in seq_peers:
            remote(buf.at[shard], buf.at[shard], kv_send.at[n], kv_recv.at[n], where).start()
    for where in ff_peers:
        remote(gains.at[ff], gains.at[ff], few_send.at[0], few_recv.at[0], where).start()

    loads[0].wait()
    loads[1].wait()
    route = ids[...]
    onehot = (jnp.broadcast_to(route, (HD, tokens)) == iota((HD, tokens), 0)).astype(F32)
    below = (iota((tokens, tokens), 0) < iota((tokens, tokens), 1)).astype(BF16)
    earlier = dot(onehot.astype(BF16), below)
    slot = jnp.sum(earlier * onehot, axis=0, keepdims=True).astype(jnp.int32)
    gate_in = as_column(jax.nn.sigmoid(logit[...]))
    gate_hi = gate_in.astype(BF16).astype(F32)
    gate_lo = gate_in - gate_hi
    lane = iota((tokens, HD), 1)
    for h in range(2):
        mine = (slot >= part * h) & (slot < part * (h + 1))
        target = jnp.where(mine, route * part + slot - part * h, -1)
        choose[h] = (iota((half, tokens), 0) == target).astype(BF16)
        expert = jnp.where(mine, route, -1)
        owner[h] = (iota((n_exp, tokens), 0) == expert).astype(BF16)
        place = as_column((slot - part * h).astype(F32)).astype(jnp.int32)
        metas[h] = jnp.where(
            lane == place, gate_hi, jnp.where(lane == place + HD // 2, gate_lo, 0.0)
        ).astype(BF16)

    def dense_row(r):
        in_block = r & (ROWS - 1)
        b = (in_block * 11) >> 5
        row = b * (lot * part) + (r >> 4) * part + in_block - part * b
        return jnp.where(in_block < ROWS - 1, row, cols * lot * part + (r >> 4))

    lot_rows = lot * ROWS
    dense_rows = (cols * part + 1) * lot
    keep[...] = (
        iota((dense_rows, lot_rows), 0) == dense_row(iota((dense_rows, lot_rows), 1))
    ).astype(BF16)
    widen[...] = (
        iota((lot_rows, dense_rows), 1) == dense_row(iota((lot_rows, dense_rows), 0))
    ).astype(BF16)
    acc[...] = jnp.zeros_like(acc)
    sq[...] = jnp.zeros_like(sq)

    def to_blocks(target, h, dense, extra):
        for n in range(0, n_exp, lot):
            stack = [dense[n * part : (n + lot) * part, b * HD : (b + 1) * HD] for b in range(cols)]
            stack = jnp.concatenate(stack + [extra[n : n + lot]], axis=0)
            block = dot(widen[...], stack).astype(BF16)
            target[h, n : n + lot] = block.reshape(lot, ROWS, HD)

    def from_blocks(source, h, n):
        return dot(keep[...], source[h, n : n + lot].reshape(lot_rows, HD)).astype(BF16)

    loads[5].wait()
    loads[6].wait()

    span = 4 * tokens
    group = HEADS // KVH
    pltpu.make_async_copy(kbuf.at[0:3], kbuf.at[0:3], kv_recv.at[0]).wait()
    pltpu.make_async_copy(vbuf.at[0:3], vbuf.at[0:3], kv_recv.at[1]).wait()
    allowed = iota((tokens, span), 1) <= iota((tokens, span), 0) + shard * tokens
    for a in range(kbuf.shape[2] // HD):
        keys = kbuf[:, :, a * HD : (a + 1) * HD].reshape(span, HD)
        values = vbuf[:, :, a * HD : (a + 1) * HD].reshape(span, HD)
        for g in range(group):
            h = (a * group + g) * HD
            scores = dot_cols(query[:, h : h + HD], keys) * HD ** (-0.5)
            scores = jnp.where(allowed, scores, FLOOR)
            peak = jnp.max(scores, axis=-1, keepdims=True)
            weights = jnp.where(allowed, jnp.exp(scores - peak), 0.0)
            total = jnp.sum(weights, axis=-1, keepdims=True)
            mixed = dot(weights.astype(BF16), values) / total
            stream[:, h : h + HD] = (res[:, h : h + HD].astype(F32) + mixed).astype(BF16)

    def a2a_copy(h, k):
        to = lax.rem(exp + k, n_exp)
        return remote(packed.at[h, to], landed.at[h, exp], a2a_send.at[h], a2a_recv.at[h], {"exp": to})

    for h in range(2):
        dense = dot(choose[h], stream[...]).astype(BF16)
        to_blocks(packed, h, dense, dot(owner[h], metas[h]).astype(BF16))
        landed[h, exp] = packed[h, exp]

        def a2a_start(k, carry):
            a2a_copy(h, k).start()
            return carry

        lax.fori_loop(1, n_exp, a2a_start, 0)

    for n in range(7, 10):
        loads[n].wait()
    pltpu.make_async_copy(gains.at[0 : n_ff - 1], gains.at[0 : n_ff - 1], few_recv.at[0]).wait()

    def fold(b, carry):
        f = b // cols
        r = b - f * cols
        column = as_column(gains[f, pl.ds(r, 1), :])
        src = pl.ds(pl.multiple_of(b * HD, HD), HD)
        dst = pl.ds(pl.multiple_of(r * HD, HD), HD)
        wgu[f, dst, 0:hidden] = (wg_raw[src, :].astype(F32) * column).astype(BF16)
        wgu[f, dst, hidden : 2 * hidden] = (wu_raw[src, :].astype(F32) * column).astype(BF16)
        return carry

    lax.fori_loop(0, n_ff * cols, fold, 0)
    def a2a_landed(h):
        some = pl.ds(0, n_exp - 1)
        pltpu.make_async_copy(packed.at[h, some], landed.at[h, some], a2a_recv.at[h]).wait()

    def own_dense(h):
        with jax.named_scope(f"land#h={h}"):
            a2a_landed(h)
        for n in range(0, n_exp, lot):
            dense = from_blocks(landed, h, n)
            for b in range(cols):
                xbuf[zeta, core, h, n * part : (n + lot) * part, b * HD : (b + 1) * HD] = dense[
                    b * lot * part : (b + 1) * lot * part
                ]
            sigs[shard, h, n : n + lot] = dense[cols * lot * part :]

    quarter = half // 2

    def quarter_of(v):
        return pl.ds(v * quarter, quarter)

    def ring_item(d, p):
        k = p // 2 + 1
        z = lax.rem((zeta - k if d == 0 else zeta + k) + n_ring, n_ring)
        h = lax.rem(p, 2)
        return z, (h if d == 0 else jnp.where(p == items - 1, 1, h))

    def ag_copy(d, p, v, z, h):
        ref = xbuf.at[z, core, h, quarter_of(v)]
        return remote(ref, ref, ring_send.at[0], ag_recv.at[d, p, v], nxt[d])

    def own_copy(c, h):
        ref = xbuf.at[zeta, c, h]
        return remote(ref, ref, ring_send.at[1], own_recv.at[h], sibling)

    def fwd_copy(d, p, z, c, h):
        ref = xbuf.at[z, c, h]
        return remote(ref, ref, ring_send.at[2], fwd_recv.at[d, p], sibling)

    def multiply(z, c, h):
        x = xbuf[z, c, h]
        s = lax.rem(z, 2) * 2 + c
        acc[s, h] += dot(x, wgu[z // 2])
        squares = None
        for b in range(cols):
            xf = x[:, b * HD : (b + 1) * HD].astype(F32)
            squares = xf * xf if squares is None else squares + xf * xf
        sq[s, h] += squares

    for h in range(2):
        own_dense(h)
        own_copy(core, h).start()
        for v in range(2):
            for d in range(2):
                ag_copy(d, h, v, zeta, h).start()
        if h == 0:
            multiply(zeta, core, h)

    for where in seq_peers:
        remote(sigs.at[shard], sigs.at[shard], few_send.at[1], few_recv.at[1], where).start()

    multiply(zeta, core, 1)

    def from_sibling(p):
        for d in range(2):
            z, h = ring_item(d, p)
            fwd_copy(d, p, z, 1 - core, h).wait_recv()
            multiply(z, 1 - core, h)

    def gather_step(p, carry):
        for v in range(2):
            for d in range(2):
                z, h = ring_item(d, p)
                with jax.named_scope(f"arrive#v={v}#d={d}"):
                    ag_copy(d, p, v, z, h).wait_recv()
                if d == 0:

                    @pl.when(p < items - 2)
                    def _():
                        ag_copy(d, p + 2, v, z, h).start()

                else:

                    @pl.when(p < items - 3)
                    def _():
                        ag_copy(d, p + 2, v, z, h).start()

                    @pl.when(p == items - 2)
                    def _():
                        ag_copy(d, p + 1, v, z, h).start()

        for d in range(2):
            z, h = ring_item(d, p)
            fwd_copy(d, p, z, core, h).start()
        for d in range(2):
            z, h = ring_item(d, p)
            multiply(z, core, h)

        @pl.when(p >= LAG)
        def _():
            from_sibling(p - LAG)

        return carry

    lax.fori_loop(0, LAG, gather_step, 0)
    for h in range(2):
        own_copy(1 - core, h).wait_recv()
        multiply(zeta, 1 - core, h)
    lax.fori_loop(LAG, items, gather_step, 0)
    for p in range(items - LAG, items):
        from_sibling(p)

    pltpu.make_async_copy(sigs.at[0:3], sigs.at[0:3], few_recv.at[1]).wait()
    first = part * iota((half, n_exp), 1)
    spread = (iota((half, n_exp), 0) >= first) & (iota((half, n_exp), 0) < first + part)
    spread = spread.astype(BF16)
    r_lane = iota((half, HD), 0)
    here = (r_lane - part * ((r_lane * 171) >> 9)) == (iota((half, HD), 1) & (HD // 2 - 1))
    for h in range(2):
        for s in range(4):
            sig = jnp.sum(jnp.where(here, dot(spread, sigs[s, h]), 0.0), axis=1, keepdims=True)
            meansq = jnp.sum(sq[s, h], axis=1, keepdims=True) / D
            factor = lax.rsqrt(meansq + NORM_EPS) * sig
            gate = acc[s, h, :, 0:hidden] * factor
            up = acc[s, h, :, hidden : 2 * hidden] * factor
            act[s, h] = (gate / (1.0 + jnp.exp(-gate)) * up).astype(BF16)

    def partial(z, c, h):
        s = lax.rem(z, 2) * 2 + c
        return dot(act[s, h], wd[:, pl.ds(pl.multiple_of((z // 2) * width, HD), width)])

    def rs_target(d, p):
        k = n_ff - (p + 1) // 2
        z = lax.rem((zeta + k if d == 0 else zeta - k) + n_ring, n_ring)
        h = lax.rem(p + 1, 2)
        return z, (jnp.where(p == 0, 0, h) if d == 0 else h)

    def sp_copy(d, p):
        return remote(sib_out.at[d, p], sib_in.at[d, p], ring_send.at[3], sp_recv.at[d, p], sibling)

    def for_sibling(p):
        for d in range(2):
            z, h = rs_target(d, p)
            sib_out[d, p] = partial(z, 1 - core, h).astype(BF16)
        for d in range(2):
            sp_copy(d, p).start()

    def rs_copy(d, p, v):
        return remote(
            rs_out.at[d, p, quarter_of(v)],
            rs_in.at[d, p, quarter_of(v)],
            ring_send.at[4],
            rs_recv.at[d, p, v],
            nxt[d],
        )

    def scatter_step(p, before):
        mine = []
        for d in range(2):
            z, h = rs_target(d, p)
            own = partial(z, core, h)
            sp_copy(d, p).wait_recv()
            mine.append(own + sib_in[d, p].astype(F32))
        for v in range(2):
            rows = quarter_of(v)
            for d in range(2):
                block = mine[d][v * quarter : (v + 1) * quarter]
                if before[d] is not None:
                    rs_copy(d, before[d], v).wait_recv()
                    block = block + rs_in[d, before[d], rows].astype(F32)
                rs_out[d, p, rows] = block.astype(BF16)
            for d in range(2):
                rs_copy(d, p, v).start()

    def chained_step(p, carry):
        scatter_step(p, (p - 2, p - 2))
        return carry

    for_sibling(0)
    for_sibling(1)
    scatter_step(0, (None, None))
    for_sibling(2)
    for_sibling(3)
    scatter_step(1, (0, None))
    for_sibling(4)
    for_sibling(5)
    scatter_step(2, (None, 0))
    for_sibling(6)
    for h in range(2):
        sib_out[h, items] = partial(zeta, 1 - core, h).astype(BF16)
    for h in range(2):
        sp_copy(h, items).start()
    lax.fori_loop(3, items, chained_step, 0)

    def bk_copy(h, k):
        to = lax.rem(exp + k, n_exp)
        return remote(back_out.at[h, to], back_in.at[h, exp], bk_send.at[h], bk_recv.at[h], {"exp": to})

    finals = [partial(zeta, core, h) for h in range(2)]
    for h in range(2):
        sp_copy(h, items).wait_recv()
        finals[h] = finals[h] + sib_in[h, items].astype(F32)
    blank = jnp.zeros((n_exp, HD), BF16)
    for h in range(2):
        p = items - 2 + h
        for d in range(2):
            for v in range(2):
                rs_copy(d, p, v).wait_recv()
        dense = finals[h] + rs_in[0, p].astype(F32) + rs_in[1, p].astype(F32)
        to_blocks(back_out, h, dense.astype(BF16), blank)
        back_in[h, exp] = back_out[h, exp]

        def bk_start(k, carry):
            bk_copy(h, k).start()
            return carry

        lax.fori_loop(1, n_exp, bk_start, 0)

    def sent(ref, sem):
        pltpu.make_async_copy(ref, ref, sem).wait()

    for n, buf in enumerate((kbuf, vbuf)):
        sent(buf.at[0:3], kv_send.at[n])
    sent(gains.at[0 : n_ff - 1], few_send.at[0])
    sent(sigs.at[0:3], few_send.at[1])
    for n in (0, 2, 4):
        sent(rs_out, ring_send.at[n])
    sent(xbuf.at[0, 0], ring_send.at[1])
    sent(sib_out, ring_send.at[3])
    for h in range(2):
        sent(packed.at[h, pl.ds(0, n_exp - 1)], a2a_send.at[h])

    total = None
    for h in range(2):
        some = pl.ds(0, n_exp - 1)
        pltpu.make_async_copy(back_out.at[h, some], back_in.at[h, some], bk_recv.at[h]).wait()
        lots = [from_blocks(back_in, h, n) for n in range(0, n_exp, lot)]
        step = lot * part
        dense = [
            jnp.concatenate([x[b * step : (b + 1) * step] for x in lots], axis=0) for b in range(cols)
        ]
        picked = dot_rows(choose[h], jnp.concatenate(dense, axis=1))
        total = picked if total is None else total + picked

    out_ref[...] = (stream[...].astype(F32) + total).astype(BF16)
    for h in range(2):
        sent(back_out.at[h, pl.ds(0, n_exp - 1)], bk_send.at[h])


def run_layer(n_exp, n_ff, key, value, ids, logit, gain, query, residual, wg, wu, wd):
    tokens, width = query.shape
    hidden = wg.shape[1]
    items = 2 * n_ff - 1
    cols = width // HD
    half = n_exp * CAP // 2
    lot_rows = min(n_exp, LOT) * ROWS
    dense_rows = (cols * CAP // 2 + 1) * min(n_exp, LOT)
    dma = pltpu.SemaphoreType.DMA

    def kernel(*refs):
        layer_kernel(n_exp, n_ff, *refs)

    def like(x):
        return pltpu.VMEM(x.shape, x.dtype)

    blocks = pltpu.VMEM((2, n_exp, ROWS, HD), BF16)
    return pl.pallas_call(
        kernel,
        out_shape=pltpu.VMEM((tokens, width), BF16),
        in_specs=[pl.BlockSpec(memory_space=pl.ANY)] * 10,
        out_specs=pl.BlockSpec(memory_space=pltpu.VMEM),
        scratch_shapes=[
            pltpu.VMEM((4, *key.shape), BF16),
            pltpu.VMEM((4, *value.shape), BF16),
            like(ids),
            like(logit),
            pltpu.VMEM((n_ff, *gain.shape), F32),
            like(query),
            like(residual),
            like(wg),
            like(wu),
            like(wd),
            pltpu.VMEM((n_ff, width, 2 * hidden), BF16),
            pltpu.VMEM((tokens, width), BF16),
            pltpu.VMEM((2, half, tokens), BF16),
            pltpu.VMEM((2, n_exp, tokens), BF16),
            pltpu.VMEM((2, tokens, HD), BF16),
            pltpu.VMEM((dense_rows, lot_rows), BF16),
            pltpu.VMEM((lot_rows, dense_rows), BF16),
            blocks,
            blocks,
            pltpu.VMEM((4, 2, n_exp, HD), BF16),
            pltpu.VMEM((2 * n_ff, 2, 2, half, width), BF16),
            pltpu.VMEM((4, 2, half, 2 * hidden), F32),
            pltpu.VMEM((4, 2, half, HD), F32),
            pltpu.VMEM((4, 2, half, hidden), BF16),
            pltpu.VMEM((2, items + 1, half, width), BF16),
            pltpu.VMEM((2, items + 1, half, width), BF16),
            pltpu.VMEM((2, items, half, width), BF16),
            pltpu.VMEM((2, items, half, width), BF16),
            blocks,
            blocks,
            dma((10,)),
            dma((2,)),
            dma((2,)),
            dma((2,)),
            dma((2,)),
            dma((2,)),
            dma((2,)),
            dma((5,)),
            dma((2, items, 2)),
            dma((2,)),
            dma((2, items)),
            dma((2, items + 1)),
            dma((2, items, 2)),
            dma((2,)),
            dma((2,)),
        ],
        compiler_params=pltpu.CompilerParams(
            collective_id=0, has_side_effects=True, vmem_limit_bytes=60 * 1024 * 1024
        ),
        name="layer",
    )(key, value, ids, logit, gain, query, residual, wg, wu, wd)


def solution(mesh):
    n_exp, n_ff = mesh.shape["exp"], mesh.shape["ff"]
    torus = Mesh(mesh.devices.reshape(2, 2, n_exp, n_ff), ("zl", "core", "exp", "ff"))

    def body(query, key, value, residual, gain, logit, ids, wg, wu, wd):
        out = run_layer(
            n_exp,
            n_ff,
            key[0],
            value[0],
            ids.reshape(1, -1),
            logit,
            gain.reshape(-1, HD),
            query[0],
            residual[0],
            wg[0],
            wu[0],
            wd[0],
        )
        return out[None]

    placed = (
        P("exp", SEQ, "ff"),
        P("exp", SEQ, "ff"),
        P("exp", SEQ, "ff"),
        P("exp", SEQ, "ff"),
        P("ff"),
        P("exp", SEQ),
        P("exp", SEQ, None),
        P("exp", None, SEQ_FF),
        P("exp", None, SEQ_FF),
        P("exp", SEQ_FF, None),
    )
    return jax.shard_map(
        body, mesh=torus, in_specs=placed, out_specs=P("exp", SEQ, "ff"), check_vma=False
    )
```

```python
import jax
import jax.numpy as jnp
from jax import lax
from jax.experimental import pallas as pl
from jax.experimental.pallas import tpu as pltpu
from jax.sharding import Mesh
from jax.sharding import PartitionSpec as P

HD = 128
HEADS = 20
KVH = 4
D = 2560
CAP = 6
ROWS = 16
LOT = 16
LAG = 2
SEQ = ("zl", "core")
SEQ_FF = ("zl", "core", "ff")
NORM_EPS = 1e-05
FLOOR = -1e30
BF16 = jnp.bfloat16
F32 = jnp.float32
MESH = pl.DeviceIdType.MESH


AG_ORDER = (
    [(p, v) for p in range(7) for v in range(2)],
    [(p, v) for p in range(4) for v in range(2)] + [(4, 0), (5, 0), (5, 1), (4, 1), (6, 0), (6, 1)],
)
AG_ONWARD = (
    {(p, v): ((p, v, p + 2),) for p in range(5) for v in range(2)},
    {
        **{(p, v): ((p, v, p + 2),) for p in range(2) for v in range(2)},
        (2, 0): ((2, 0, 4),),
        (3, 0): ((3, 0, 5),),
        (3, 1): ((3, 1, 5), (2, 1, 4)),
        (5, 0): ((5, 0, 6),),
        (5, 1): ((5, 1, 6),),
    },
)
AG_WHOLE = [[(0, p), (1, p)] for p in range(4)] + [[(0, 4)], [(0, 5), (1, 5), (1, 4)], [(0, 6), (1, 6)]]
RS_ORDER = (
    [(2, 0), (2, 1), (0, 0), (0, 1), (4, 0), (1, 0), (1, 1), (4, 1), (3, 0), (3, 1), (6, 0), (5, 0), (5, 1), (6, 1)],
    [(1, 0), (1, 1), (0, 0), (0, 1), (3, 0), (2, 0), (2, 1), (3, 1), (4, 0), (4, 1), (5, 0), (5, 1), (6, 0), (6, 1)],
)
RS_BEFORE = ({1: 0, 3: 1, 5: 3, 4: 2, 6: 4}, {2: 0, 4: 2, 6: 4, 3: 1, 5: 3})
RS_GROUPS = ((2, 1), (0, 0), (4, 3), (1, 2), (3, 4), (6, 5), (5, 6))


def remote(src, dst, send, recv, where):
    return pltpu.make_async_remote_copy(
        src_ref=src, dst_ref=dst, send_sem=send, recv_sem=recv, device_id=where, device_id_type=MESH
    )


def dot(a, b):
    return jnp.dot(a, b, preferred_element_type=F32)


def dot_rows(a, b):
    return lax.dot_general(a, b, (((0,), (0,)), ((), ())), preferred_element_type=F32)


def dot_cols(a, b):
    return lax.dot_general(a, b, (((1,), (1,)), ((), ())), preferred_element_type=F32)


def iota(shape, dim):
    return lax.broadcasted_iota(jnp.int32, shape, dim)


def as_column(row):
    n = row.shape[-1]
    eye = iota((n, n), 0) == iota((n, n), 1)
    return jnp.sum(jnp.where(eye, jnp.broadcast_to(row, (n, n)), 0.0), axis=1, keepdims=True)


def far_first(n_exp):
    ny = min(n_exp, 8)
    nx = n_exp // ny
    offsets = [(dx, dy) for dx in range(nx) for dy in range(ny) if dx or dy]
    return sorted(offsets, key=lambda o: -(min(o[0], nx - o[0]) + min(o[1], ny - o[1]))), nx, ny


def layer_kernel(
    n_exp,
    n_ff,
    k_hbm,
    v_hbm,
    ids_hbm,
    logit_hbm,
    gain_hbm,
    q_hbm,
    res_hbm,
    wg_hbm,
    wu_hbm,
    wd_hbm,
    out_ref,
    kbuf,
    vbuf,
    ids,
    logit,
    gains,
    query,
    res,
    wg_raw,
    wu_raw,
    wd,
    wgu,
    stream,
    choose,
    owner,
    metas,
    keep,
    widen,
    packed,
    landed,
    sigs,
    xbuf,
    acc,
    sq,
    act,
    sib_out,
    sib_in,
    rs_out,
    rs_in,
    mine,
    back_out,
    back_in,
    load_sem,
    kv_send,
    kv_recv,
    few_send,
    few_recv,
    a2a_send,
    a2a_recv,
    ring_send,
    ag_recv,
    own_recv,
    fwd_recv,
    sp_recv,
    rs_recv,
    bk_send,
    bk_recv,
):
    n_ring = 2 * n_ff
    items = n_ring - 1
    zl, core = lax.axis_index("zl"), lax.axis_index("core")
    exp, ff = lax.axis_index("exp"), lax.axis_index("ff")
    shard = zl * 2 + core
    zeta = ff * 2 + zl
    tokens, width = query.shape
    cols = width // HD
    part = CAP // 2
    half = n_exp * part
    hidden = wg_raw.shape[1]
    lot = min(n_exp, LOT)

    def at_ring(step):
        z = lax.rem(zeta + step + n_ring, n_ring)
        return {"zl": lax.rem(z, 2), "ff": z // 2}

    sibling = {"core": 1 - core}
    seq_peers = ({"zl": 1 - zl, "core": 1 - core}, {"zl": 1 - zl}, sibling)
    nxt = (at_ring(1), at_ring(-1))
    ff_peers = [{"ff": lax.rem(ff + k, n_ff)} for k in range(1, n_ff)]

    offsets, nx, ny = far_first(n_exp)
    exp_x, exp_y = exp // ny, lax.rem(exp, ny)

    def partner(offset):
        dx, dy = offset
        return lax.rem(exp_x + dx, nx) * ny + lax.rem(exp_y + dy, ny)

    loads = [
        pltpu.make_async_copy(src, dst, load_sem.at[n])
        for n, (src, dst) in enumerate(
            (
                (ids_hbm, ids),
                (logit_hbm, logit),
                (k_hbm, kbuf.at[shard]),
                (v_hbm, vbuf.at[shard]),
                (gain_hbm, gains.at[ff]),
                (q_hbm, query),
                (res_hbm, res),
                (wg_hbm, wg_raw),
                (wu_hbm, wu_raw),
                (wd_hbm, wd),
            )
        )
    ]
    for load in loads:
        load.start()
    barrier = pltpu.get_barrier_semaphore()
    greeted = [sibling, {"zl": 1 - zl, "core": 1 - core}, *nxt]
    for where in greeted + ff_peers:
        pl.semaphore_signal(barrier, inc=1, device_id=where, device_id_type=MESH)

    for offset in offsets:
        pl.semaphore_signal(
            barrier, inc=1, device_id={"exp": partner(offset)}, device_id_type=MESH
        )
    loads[2].wait()
    loads[3].wait()
    loads[4].wait()

    pl.semaphore_wait(barrier, n_exp - 1 + len(greeted) + len(ff_peers))
    for n, buf in enumerate((kbuf, vbuf)):
        for where in seq_peers:
            remote(buf.at[shard], buf.at[shard], kv_send.at[n], kv_recv.at[n], where).start()
    for where in ff_peers:
        remote(gains.at[ff], gains.at[ff], few_send.at[0], few_recv.at[0], where).start()

    loads[0].wait()
    loads[1].wait()
    route = ids[...]
    onehot = (jnp.broadcast_to(route, (HD, tokens)) == iota((HD, tokens), 0)).astype(F32)
    below = (iota((tokens, tokens), 0) < iota((tokens, tokens), 1)).astype(BF16)
    earlier = dot(onehot.astype(BF16), below)
    slot = jnp.sum(earlier * onehot, axis=0, keepdims=True).astype(jnp.int32)
    gate_in = as_column(jax.nn.sigmoid(logit[...]))
    gate_hi = gate_in.astype(BF16).astype(F32)
    gate_lo = gate_in - gate_hi
    lane = iota((tokens, HD), 1)
    for h in range(2):
        inside = (slot >= part * h) & (slot < part * (h + 1))
        target = jnp.where(inside, route * part + slot - part * h, -1)
        choose[h] = (iota((half, tokens), 0) == target).astype(BF16)
        expert = jnp.where(inside, route, -1)
        owner[h] = (iota((n_exp, tokens), 0) == expert).astype(BF16)
        place = as_column((slot - part * h).astype(F32)).astype(jnp.int32)
        metas[h] = jnp.where(
            lane == place, gate_hi, jnp.where(lane == place + HD // 2, gate_lo, 0.0)
        ).astype(BF16)

    def dense_row(r):
        in_block = r & (ROWS - 1)
        b = (in_block * 11) >> 5
        row = b * (lot * part) + (r >> 4) * part + in_block - part * b
        return jnp.where(in_block < ROWS - 1, row, cols * lot * part + (r >> 4))

    lot_rows = lot * ROWS
    dense_rows = (cols * part + 1) * lot
    keep[...] = (
        iota((dense_rows, lot_rows), 0) == dense_row(iota((dense_rows, lot_rows), 1))
    ).astype(BF16)
    widen[...] = (
        iota((lot_rows, dense_rows), 1) == dense_row(iota((lot_rows, dense_rows), 0))
    ).astype(BF16)
    acc[...] = jnp.zeros_like(acc)
    sq[...] = jnp.zeros_like(sq)

    def to_blocks(target, h, dense, extra):
        for n in range(0, n_exp, lot):
            stack = [dense[n * part : (n + lot) * part, b * HD : (b + 1) * HD] for b in range(cols)]
            stack = jnp.concatenate(stack + [extra[n : n + lot]], axis=0)
            block = dot(widen[...], stack).astype(BF16)
            target[h, n : n + lot] = block.reshape(lot, ROWS, HD)

    def from_blocks(source, h, n):
        return dot(keep[...], source[h, n : n + lot].reshape(lot_rows, HD)).astype(BF16)

    loads[5].wait()
    loads[6].wait()

    span = 4 * tokens
    group = HEADS // KVH
    pltpu.make_async_copy(kbuf.at[0:3], kbuf.at[0:3], kv_recv.at[0]).wait()
    pltpu.make_async_copy(vbuf.at[0:3], vbuf.at[0:3], kv_recv.at[1]).wait()
    allowed = iota((tokens, span), 1) <= iota((tokens, span), 0) + shard * tokens
    for a in range(kbuf.shape[2] // HD):
        keys = kbuf[:, :, a * HD : (a + 1) * HD].reshape(span, HD)
        values = vbuf[:, :, a * HD : (a + 1) * HD].reshape(span, HD)
        for g in range(group):
            h = (a * group + g) * HD
            scores = dot_cols(query[:, h : h + HD], keys) * HD ** (-0.5)
            scores = jnp.where(allowed, scores, FLOOR)
            peak = jnp.max(scores, axis=-1, keepdims=True)
            weights = jnp.where(allowed, jnp.exp(scores - peak), 0.0)
            total = jnp.sum(weights, axis=-1, keepdims=True)
            mixed = dot(weights.astype(BF16), values) / total
            stream[:, h : h + HD] = (res[:, h : h + HD].astype(F32) + mixed).astype(BF16)

    def a2a_copy(h, offset):
        to = partner(offset)
        return remote(packed.at[h, to], landed.at[h, exp], a2a_send.at[h], a2a_recv.at[h], {"exp": to})

    dense = dot(choose[...].reshape(2 * half, tokens), stream[...]).astype(BF16)
    extra = [dot(owner[h], metas[h]).astype(BF16) for h in range(2)]
    for n in range(0, n_exp, lot):
        sides = []
        for h in range(2):
            at = h * half + n * part
            stack = [dense[at : at + lot * part, b * HD : (b + 1) * HD] for b in range(cols)]
            sides.append(jnp.concatenate(stack + [extra[h][n : n + lot]], axis=0))
        block = dot(widen[...], jnp.concatenate(sides, axis=1)).astype(BF16)
        for h in range(2):
            packed[h, n : n + lot] = block[:, h * HD : (h + 1) * HD].reshape(lot, ROWS, HD)
    for h in range(2):
        landed[h, exp] = packed[h, exp]
        for offset in offsets:
            a2a_copy(h, offset).start()

    for n in range(7, 10):
        loads[n].wait()
    pltpu.make_async_copy(gains.at[0 : n_ff - 1], gains.at[0 : n_ff - 1], few_recv.at[0]).wait()

    def fold(b, carry):
        f = b // cols
        r = b - f * cols
        column = as_column(gains[f, pl.ds(r, 1), :])
        src = pl.ds(pl.multiple_of(b * HD, HD), HD)
        dst = pl.ds(pl.multiple_of(r * HD, HD), HD)
        wgu[f, dst, 0:hidden] = (wg_raw[src, :].astype(F32) * column).astype(BF16)
        wgu[f, dst, hidden : 2 * hidden] = (wu_raw[src, :].astype(F32) * column).astype(BF16)
        return carry

    lax.fori_loop(0, n_ff * cols, fold, 0)
    def a2a_landed(h):
        some = pl.ds(0, n_exp - 1)
        pltpu.make_async_copy(packed.at[h, some], landed.at[h, some], a2a_recv.at[h]).wait()

    def own_dense(h):
        with jax.named_scope(f"land#h={h}"):
            a2a_landed(h)
        for n in range(0, n_exp, lot):
            dense = from_blocks(landed, h, n)
            for b in range(cols):
                xbuf[zeta, core, h, n * part : (n + lot) * part, b * HD : (b + 1) * HD] = dense[
                    b * lot * part : (b + 1) * lot * part
                ]
            sigs[shard, h, n : n + lot] = dense[cols * lot * part :]

    quarter = half // 2

    def quarter_of(v):
        return pl.ds(v * quarter, quarter)

    def ring_item(d, p):
        k = p // 2 + 1
        z = lax.rem((zeta - k if d == 0 else zeta + k) + n_ring, n_ring)
        return z, (1 if d == 1 and p == items - 1 else p % 2)

    def ag_copy(d, p, v, z, h):
        ref = xbuf.at[z, core, h, quarter_of(v)]
        return remote(ref, ref, ring_send.at[0], ag_recv.at[d, p, v], nxt[d])

    def own_copy(c, h):
        ref = xbuf.at[zeta, c, h]
        return remote(ref, ref, ring_send.at[1], own_recv.at[h], sibling)

    def fwd_copy(d, p, z, c, h):
        ref = xbuf.at[z, c, h]
        return remote(ref, ref, ring_send.at[2], fwd_recv.at[d, p], sibling)

    def multiply(z, c, h):
        x = xbuf[z, c, h]
        s = lax.rem(z, 2) * 2 + c
        acc[s, h] += dot(x, wgu[z // 2])
        squares = None
        for b in range(cols):
            xf = x[:, b * HD : (b + 1) * HD].astype(F32)
            squares = xf * xf if squares is None else squares + xf * xf
        sq[s, h] += squares

    for h in range(2):
        own_dense(h)
        own_copy(core, h).start()
        for v in range(2):
            for d in range(2):
                ag_copy(d, h, v, zeta, h).start()
        if h == 0:
            multiply(zeta, core, h)

    for where in seq_peers:
        remote(sigs.at[shard], sigs.at[shard], few_send.at[1], few_recv.at[1], where).start()

    multiply(zeta, core, 1)

    def from_sibling(d, p):
        z, h = ring_item(d, p)
        fwd_copy(d, p, z, 1 - core, h).wait_recv()
        multiply(z, 1 - core, h)

    def onward(d, p, v, to):
        z, h = ring_item(d, p)
        ag_copy(d, to, v, z, h).start()

    def take(slot):
        for n in (2 * slot, 2 * slot + 1):
            for d in range(2):
                p, v = AG_ORDER[d][n]
                z, h = ring_item(d, p)
                ag_copy(d, p, v, z, h).wait_recv()
                for p_on, v_on, to in AG_ONWARD[d].get((p, v), ()):
                    onward(d, p_on, v_on, to)
        for d, p in AG_WHOLE[slot]:
            z, h = ring_item(d, p)
            fwd_copy(d, p, z, core, h).start()
        for d, p in AG_WHOLE[slot]:
            z, h = ring_item(d, p)
            multiply(z, core, h)

    for slot in range(items - 1):
        take(slot)
        if slot == 1:
            for h in range(2):
                own_copy(1 - core, h).wait_recv()
                multiply(zeta, 1 - core, h)
        if slot >= LAG:
            for d, p in AG_WHOLE[slot - LAG]:
                from_sibling(d, p)
    for slot in range(items - 1 - LAG, items - 1):
        for d, p in AG_WHOLE[slot]:
            from_sibling(d, p)

    pltpu.make_async_copy(sigs.at[0:3], sigs.at[0:3], few_recv.at[1]).wait()
    first = part * iota((half, n_exp), 1)
    spread = (iota((half, n_exp), 0) >= first) & (iota((half, n_exp), 0) < first + part)
    spread = spread.astype(BF16)
    r_lane = iota((half, HD), 0)
    here = (r_lane - part * ((r_lane * 171) >> 9)) == (iota((half, HD), 1) & (HD // 2 - 1))

    def activate(z_part):
        for c in range(2):
            s = z_part * 2 + c
            for h in range(2):
                sig = jnp.sum(jnp.where(here, dot(spread, sigs[s, h]), 0.0), axis=1, keepdims=True)
                meansq = jnp.sum(sq[s, h], axis=1, keepdims=True) / D
                factor = lax.rsqrt(meansq + NORM_EPS) * sig
                gate = acc[s, h, :, 0:hidden] * factor
                up = acc[s, h, :, hidden : 2 * hidden] * factor
                act[s, h] = (gate / (1.0 + jnp.exp(-gate)) * up).astype(BF16)

    def partial(z, c, h):
        s = lax.rem(z, 2) * 2 + c
        return dot(act[s, h], wd[:, pl.ds(pl.multiple_of((z // 2) * width, HD), width)])

    def rs_target(d, p):
        k = n_ff - (p + 1) // 2
        z = lax.rem((zeta + k if d == 0 else zeta - k) + n_ring, n_ring)
        return z, (0 if d == 0 and p == 0 else (p + 1) % 2)

    def sp_copy(d, p):
        return remote(sib_out.at[d, p], sib_in.at[d, p], ring_send.at[3], sp_recv.at[d, p], sibling)

    def for_sibling(group):
        for d in range(2):
            z, h = rs_target(d, RS_GROUPS[group][d])
            sib_out[d, RS_GROUPS[group][d]] = partial(z, 1 - core, h).astype(BF16)
        for d in range(2):
            sp_copy(d, RS_GROUPS[group][d]).start()

    def prepare(group):
        for d in range(2):
            p = RS_GROUPS[group][d]
            z, h = rs_target(d, p)
            own = partial(z, core, h)
            sp_copy(d, p).wait_recv()
            mine[d, p] = own + sib_in[d, p].astype(F32)

    def rs_copy(d, p, v):
        return remote(
            rs_out.at[d, p, quarter_of(v)],
            rs_in.at[d, p, quarter_of(v)],
            ring_send.at[4],
            rs_recv.at[d, p, v],
            nxt[d],
        )

    def pass_on(*slots):
        for n in slots:
            for d in range(2):
                p, v = RS_ORDER[d][n]
                rows = quarter_of(v)
                block = mine[d, p, rows]
                if p in RS_BEFORE[d]:
                    before = RS_BEFORE[d][p]
                    rs_copy(d, before, v).wait_recv()
                    block = block + rs_in[d, before, rows].astype(F32)
                rs_out[d, p, rows] = block.astype(BF16)
            for d in range(2):
                p, v = RS_ORDER[d][n]
                rs_copy(d, p, v).start()

    activate(1 - zl)
    for_sibling(0)
    prepare(0)
    pass_on(0, 1)
    take(items - 1)
    for d, p in AG_WHOLE[items - 1]:
        from_sibling(d, p)
    activate(zl)

    for_sibling(1)
    for_sibling(2)
    prepare(1)
    pass_on(2, 3)
    for_sibling(3)
    for_sibling(4)
    prepare(2)
    pass_on(4)
    for_sibling(5)
    for_sibling(6)
    prepare(3)
    pass_on(5, 6, 7)
    for h in range(2):
        sib_out[h, items] = partial(zeta, 1 - core, h).astype(BF16)
    for h in range(2):
        sp_copy(h, items).start()
    prepare(4)
    pass_on(8, 9)
    prepare(5)
    pass_on(10)
    prepare(6)
    pass_on(11, 12, 13)

    def bk_copy(h, offset):
        to = partner(offset)
        return remote(back_out.at[h, to], back_in.at[h, exp], bk_send.at[h], bk_recv.at[h], {"exp": to})

    finals = [partial(zeta, core, h) for h in range(2)]
    for h in range(2):
        sp_copy(h, items).wait_recv()
        finals[h] = finals[h] + sib_in[h, items].astype(F32)
    blank = jnp.zeros((n_exp, HD), BF16)
    for h in range(2):
        p = items - 2 + h
        for d in range(2):
            for v in range(2):
                rs_copy(d, p, v).wait_recv()
        dense = finals[h] + rs_in[0, p].astype(F32) + rs_in[1, p].astype(F32)
        to_blocks(back_out, h, dense.astype(BF16), blank)
        back_in[h, exp] = back_out[h, exp]
        for offset in offsets:
            bk_copy(h, offset).start()

    def sent(ref, sem):
        pltpu.make_async_copy(ref, ref, sem).wait()

    for n, buf in enumerate((kbuf, vbuf)):
        sent(buf.at[0:3], kv_send.at[n])
    sent(gains.at[0 : n_ff - 1], few_send.at[0])
    sent(sigs.at[0:3], few_send.at[1])
    for n in (0, 2, 4):
        sent(rs_out, ring_send.at[n])
    sent(xbuf.at[0, 0], ring_send.at[1])
    sent(sib_out, ring_send.at[3])
    for h in range(2):
        sent(packed.at[h, pl.ds(0, n_exp - 1)], a2a_send.at[h])

    total = None
    for h in range(2):
        some = pl.ds(0, n_exp - 1)
        pltpu.make_async_copy(back_out.at[h, some], back_in.at[h, some], bk_recv.at[h]).wait()
        lots = [from_blocks(back_in, h, n) for n in range(0, n_exp, lot)]
        step = lot * part
        dense = [
            jnp.concatenate([x[b * step : (b + 1) * step] for x in lots], axis=0) for b in range(cols)
        ]
        picked = dot_rows(choose[h], jnp.concatenate(dense, axis=1))
        total = picked if total is None else total + picked

    out_ref[...] = (stream[...].astype(F32) + total).astype(BF16)
    for h in range(2):
        sent(back_out.at[h, pl.ds(0, n_exp - 1)], bk_send.at[h])


def run_layer(n_exp, n_ff, key, value, ids, logit, gain, query, residual, wg, wu, wd):
    tokens, width = query.shape
    hidden = wg.shape[1]
    items = 2 * n_ff - 1
    cols = width // HD
    half = n_exp * CAP // 2
    lot_rows = min(n_exp, LOT) * ROWS
    dense_rows = (cols * CAP // 2 + 1) * min(n_exp, LOT)
    dma = pltpu.SemaphoreType.DMA

    def kernel(*refs):
        layer_kernel(n_exp, n_ff, *refs)

    def like(x):
        return pltpu.VMEM(x.shape, x.dtype)

    blocks = pltpu.VMEM((2, n_exp, ROWS, HD), BF16)
    return pl.pallas_call(
        kernel,
        out_shape=pltpu.VMEM((tokens, width), BF16),
        in_specs=[pl.BlockSpec(memory_space=pl.ANY)] * 10,
        out_specs=pl.BlockSpec(memory_space=pltpu.VMEM),
        scratch_shapes=[
            pltpu.VMEM((4, *key.shape), BF16),
            pltpu.VMEM((4, *value.shape), BF16),
            like(ids),
            like(logit),
            pltpu.VMEM((n_ff, *gain.shape), F32),
            like(query),
            like(residual),
            like(wg),
            like(wu),
            like(wd),
            pltpu.VMEM((n_ff, width, 2 * hidden), BF16),
            pltpu.VMEM((tokens, width), BF16),
            pltpu.VMEM((2, half, tokens), BF16),
            pltpu.VMEM((2, n_exp, tokens), BF16),
            pltpu.VMEM((2, tokens, HD), BF16),
            pltpu.VMEM((dense_rows, lot_rows), BF16),
            pltpu.VMEM((lot_rows, dense_rows), BF16),
            blocks,
            blocks,
            pltpu.VMEM((4, 2, n_exp, HD), BF16),
            pltpu.VMEM((2 * n_ff, 2, 2, half, width), BF16),
            pltpu.VMEM((4, 2, half, 2 * hidden), F32),
            pltpu.VMEM((4, 2, half, HD), F32),
            pltpu.VMEM((4, 2, half, hidden), BF16),
            pltpu.VMEM((2, items + 1, half, width), BF16),
            pltpu.VMEM((2, items + 1, half, width), BF16),
            pltpu.VMEM((2, items, half, width), BF16),
            pltpu.VMEM((2, items, half, width), BF16),
            pltpu.VMEM((2, items, half, width), F32),
            blocks,
            blocks,
            dma((10,)),
            dma((2,)),
            dma((2,)),
            dma((2,)),
            dma((2,)),
            dma((2,)),
            dma((2,)),
            dma((5,)),
            dma((2, items, 2)),
            dma((2,)),
            dma((2, items)),
            dma((2, items + 1)),
            dma((2, items, 2)),
            dma((2,)),
            dma((2,)),
        ],
        compiler_params=pltpu.CompilerParams(
            collective_id=0, has_side_effects=True, vmem_limit_bytes=60 * 1024 * 1024
        ),
        name="layer",
    )(key, value, ids, logit, gain, query, residual, wg, wu, wd)


def solution(mesh):
    n_exp, n_ff = mesh.shape["exp"], mesh.shape["ff"]
    torus = Mesh(mesh.devices.reshape(2, 2, n_exp, n_ff), ("zl", "core", "exp", "ff"))

    def body(query, key, value, residual, gain, logit, ids, wg, wu, wd):
        out = run_layer(
            n_exp,
            n_ff,
            key[0],
            value[0],
            ids.reshape(1, -1),
            logit,
            gain.reshape(-1, HD),
            query[0],
            residual[0],
            wg[0],
            wu[0],
            wd[0],
        )
        return out[None]

    placed = (
        P("exp", SEQ, "ff"),
        P("exp", SEQ, "ff"),
        P("exp", SEQ, "ff"),
        P("exp", SEQ, "ff"),
        P("ff"),
        P("exp", SEQ),
        P("exp", SEQ, None),
        P("exp", None, SEQ_FF),
        P("exp", None, SEQ_FF),
        P("exp", SEQ_FF, None),
    )
    return jax.shard_map(
        body, mesh=torus, in_specs=placed, out_specs=P("exp", SEQ, "ff"), check_vma=False
    )
```
